128 devices in a mesh: slab: 32 (over z, y, core), plane: 4 (over x).
Axes of the slice: x: 4, y: 4, z: 4, core: 2. Of those that a mesh axis runs over, the one named last changes fastest.
Arguments:
- tissue_v: float32 [128, 64, 128], P('slab', 'plane'), may hold values from -4 to 4
- tissue_gates: float32 [40, 128, 64, 128], P(None, 'slab', 'plane'), may hold values from 0 to 1
- tissue_diff: float32 [128, 64, 128], P('slab', 'plane'), may hold values from 0.2 to 1
- fibre_v: float32 [512, 2048], P('slab', 'plane'), may hold values from -4 to 4
- fibre_gates: float32 [40, 512, 2048], P(None, 'slab', 'plane'), may hold values from 0 to 1
- fibre_diff: float32 [512, 2048], P('slab', 'plane'), may hold values from 0.2 to 1
- gate_half: float32 [40], replicated, may hold values from -3 to 3
- gate_rate: float32 [40], replicated, may hold values from 0.5 to 20
- gate_cond: float32 [40], replicated, may hold values from 0.01 to 0.15
- gate_rev: float32 [40], replicated, may hold values from -2 to 2
- junc_cond: float32 [8], replicated, may hold values from 0.25 to 2
- junc_fibre: int32 [524288], P(('slab', 'plane')), may hold values from 0 to 15
- junc_fcell: int32 [524288], P(('slab', 'plane')), may hold values from 0 to 511
- junc_owner: int32 [524288, 1], P(('slab', 'plane')), may hold values from 0 to 127; in each aligned block of 4096 rows (0 to 4095, 4096 to 8191, ...) at most 64 rows name the same one
- junc_tcell: int32 [524288], P(('slab', 'plane')), may hold values from 0 to 8191
- junc_class: int32 [524288], P(('slab', 'plane')), may hold values from 0 to 7
Outputs:
- tissue_out: float32 [128, 64, 128], P('slab', 'plane')
- fibre_out: float32 [512, 2048], P('slab', 'plane')
The draws below stay inside these ranges and needn't reach their ends.
Inputs may be any that keep to these rules, and one draw needn't show every extreme that they name: `junc_owner`: among the junctions held by one device, no tissue block is named by more than 64 of them, and some block is named by exactly 64. `junc_fibre`: A fibre of the slab group of the device that holds the junction. `junc_fcell`: A cell of the holding device's share of that fibre. `junc_tcell`: numbered over the owner's block in the order z, y, x with x fastest.
All inputs are finite; a program needn't handle non-finite values.
Results may differ from the reference program's by a relative error of at most 0.00005.
Values sent between devices are 32-bit elements; how exact they have to be, the bound alone decides.
No kernel may reach another device: no remote copies, remote signals or barrier semaphores. Data moves between devices by JAX's collectives and lax.ppermute only.
A program may use at most 64 MiB of HBM per device.

```python
import math
import jax
import jax.numpy as jnp
import numpy as np
from jax import lax

NX = 128
CY = 16
CZ = 4
FIB_DEV = 16
FCELLS = 2048
GATES = 40
CLASSES = 8
STEPS = 14
JUNC_DEV = 4096
CAP = 64
NZ = 128
NY = 64
NFIB = 512
JUNCS = 524288
N_PLANE = 4
DEVICES = 128


def set_ends(result, own_key, least, high):
    dims = result.shape
    index_at = [jax.random.randint(jax.random.fold_in(own_key, axis), (), 0, dims[axis]) for axis in range(len(dims))]
    result = result.at[tuple(index_at)].set(least)
    longest = dims.index(max(dims))
    index_at[longest] = (index_at[longest] + 1) % dims[longest]
    return result.at[tuple(index_at)].set(high)


def block_scale(rng, dims, pieces, smallest, largest):
    gain, own = 1.0, jax.random.fold_in(rng, 6)
    for axis_at, blocks in pieces:
        draws = jnp.exp(jax.random.uniform(jax.random.fold_in(own, axis_at), (blocks,), jnp.float32, smallest / len(pieces), largest / len(pieces)))
        gain = gain * jnp.repeat(draws, dims[axis_at] // blocks).reshape([-1 if axis == axis_at else 1 for axis in range(len(dims))])
    return gain


def shared_out(rng, own, number, rows, amount, top, reach, lean):
    ranking = jax.random.permutation(rng, amount)
    packed, usual = shares(amount, rows * top, reach, lean, True), shares(amount, rows * top, reach, lean, False)
    places = jnp.arange(amount)

    def named(sizes, rotation):
        used = int((sizes > 0).sum())
        fixed = max(1, used // 4)
        moved = fixed + (places - fixed + rotation * (used - fixed)) % max(1, amount - fixed)
        return jnp.zeros((amount,), jnp.int32).at[ranking[jnp.where(places < fixed, places, moved)]].set(jnp.asarray(sizes, jnp.int32))

    sizes = jnp.where(number % 4 == 0, named(packed, number // 4), named(usual, number - number // 4 - 1))
    mixed = jax.random.permutation(jax.random.fold_in(own, 3), amount)
    giver, sink = mixed[0:amount // 2 * 2:2], mixed[1:amount // 2 * 2:2]
    room = jnp.minimum(sizes[giver] - 1, reach - sizes[sink]) // 2
    room = jnp.where((giver == ranking[0]) | (sink == ranking[0]) | (sizes[sink] == 0), 0, jnp.maximum(room, 0))
    moved = jax.random.randint(jax.random.fold_in(own, 4), (amount // 2,), 0, 1 << 20) % (room + 1)
    sizes = sizes.at[giver].add(-moved).at[sink].add(moved)
    items = jnp.searchsorted(jnp.cumsum(sizes), jnp.arange(rows * top), side="right").astype(jnp.int32)
    table = items.reshape(top, rows).T
    table = table[jax.random.permutation(jax.random.fold_in(own, 1), rows)]
    rotation = jax.random.randint(jax.random.fold_in(own, 2), (rows, 1), 0, top)
    return jnp.take_along_axis(table, (jnp.arange(top)[None, :] + rotation) % top, axis=1)


def shares(count, total, limit, lean, full):
    loads = [(1 << 20) // math.isqrt(grade ** lean) + 1 for grade in range(1, count + 1)]
    largest = limit if full else min(limit, max(-(-total // count), total * loads[0] // sum(loads)))
    least = 1 if total - largest >= count - 1 else 0
    holding, surplus = [largest] + [least] * (count - 1), total - largest - least * (count - 1)
    while surplus > 0:
        candidates = [i for i in range(1, count) if holding[i] < largest] or [i for i in range(1, count) if holding[i] < limit]
        mass, remaining = sum([loads[i] for i in candidates]), surplus
        for i in candidates:
            extra = min(limit - holding[i], max(1, remaining * loads[i] // mass), surplus)
            holding[i] = holding[i] + extra
            surplus = surplus - extra
    return np.array(holding)


def centred(rng, shape, scale, bound, split=(), kind=jnp.bfloat16):
    drawn = jax.random.normal(rng, shape, jnp.float32) * scale
    if len(split) > 0:
        drawn = block_scale(rng, shape, split, -0.22, 0.18) * drawn
    return jnp.clip(drawn, min=-bound, max=bound).astype(kind)


def setup_inputs(seed: int = 0) -> dict:
    splits = jax.random.split(jax.random.key(seed), 17)
    tissue_v = centred(splits[0], (NZ, NY, NX), 1.0, 4.0, ((0, 32), (1, 4)), jnp.float32)
    tissue_gates = jnp.clip(1.0 * jax.random.uniform(splits[1], (GATES, NZ, NY, NX), jnp.float32) ** block_scale(splits[1], (GATES, NZ, NY, NX), ((1, 32), (2, 4)), -0.2, 0.2), 0.0, 1.0)
    tissue_diff = jnp.clip(jnp.exp(math.log(1.0) - 1.609438 * jax.random.uniform(splits[2], (NZ, NY, NX), jnp.float32) ** block_scale(splits[2], (NZ, NY, NX), ((0, 32), (1, 4)), -0.2, 0.2)), 0.2, 1.0)
    fibre_v = centred(splits[3], (NFIB, FCELLS), 1.0, 4.0, ((0, 32), (1, 4)), jnp.float32)
    fibre_gates = jnp.clip(1.0 * jax.random.uniform(splits[4], (GATES, NFIB, FCELLS), jnp.float32) ** block_scale(splits[4], (GATES, NFIB, FCELLS), ((1, 32), (2, 4)), -0.2, 0.2), 0.0, 1.0)
    fibre_diff = jnp.clip(jnp.exp(math.log(1.0) - 1.609438 * jax.random.uniform(splits[5], (NFIB, FCELLS), jnp.float32) ** block_scale(splits[5], (NFIB, FCELLS), ((0, 32), (1, 4)), -0.2, 0.2)), 0.2, 1.0)
    gate_half = centred(splits[6], (GATES,), 1.0, 3.0, (), jnp.float32)
    gate_rate = jnp.clip(jnp.exp(jax.random.uniform(splits[7], (GATES,), jnp.float32, math.log(0.5), math.log(20.0))), 0.5, 20.0)
    gate_cond = jnp.clip(jnp.exp(jax.random.uniform(splits[8], (GATES,), jnp.float32, math.log(0.01), math.log(0.15))), 0.01, 0.15)
    gate_rev = jnp.clip(jax.random.uniform(splits[9], (GATES,), jnp.float32, -2.0, 2.0), -2.0, 2.0)
    junc_cond = jnp.clip(jnp.exp(jax.random.uniform(splits[10], (CLASSES,), jnp.float32, math.log(0.25), math.log(2.0))), 0.25, 2.0)
    junc_fibre = set_ends(jax.random.randint(splits[11], (JUNCS,), 0, FIB_DEV), jax.random.fold_in(splits[11], 1), 0, FIB_DEV - 1).astype(jnp.int32)
    junc_fcell = set_ends(jax.random.randint(splits[12], (JUNCS,), 0, FCELLS // N_PLANE), jax.random.fold_in(splits[12], 1), 0, (FCELLS // N_PLANE) - 1).astype(jnp.int32)
    junc_owner_keys = jax.random.split(jax.random.fold_in(splits[13], 1), JUNCS // JUNC_DEV)
    junc_owner_turns = jax.random.permutation(jax.random.fold_in(splits[13], 3), JUNCS // JUNC_DEV)
    junc_owner = jax.vmap(lambda own, number: shared_out(jax.random.fold_in(splits[13], 2), own, number, JUNC_DEV, DEVICES, 1, CAP, 2))(junc_owner_keys, junc_owner_turns).reshape((JUNCS, 1))
    junc_tcell = set_ends(jax.random.randint(splits[14], (JUNCS,), 0, CZ * CY * NX), jax.random.fold_in(splits[14], 1), 0, (CZ * CY * NX) - 1).astype(jnp.int32)
    junc_class = set_ends(jax.random.randint(splits[15], (JUNCS,), 0, CLASSES), jax.random.fold_in(splits[15], 1), 0, CLASSES - 1).astype(jnp.int32)
    return {"tissue_v": tissue_v, "tissue_gates": tissue_gates, "tissue_diff": tissue_diff, "fibre_v": fibre_v, "fibre_gates": fibre_gates, "fibre_diff": fibre_diff, "gate_half": gate_half, "gate_rate": gate_rate, "gate_cond": gate_cond, "gate_rev": gate_rev, "junc_cond": junc_cond, "junc_fibre": junc_fibre, "junc_fcell": junc_fcell, "junc_owner": junc_owner, "junc_tcell": junc_tcell, "junc_class": junc_class}


time_step = 0.1
gate_slope = 2.0


def membrane(voltage, gates, gate_half, gate_rate, gate_cond, gate_rev):
    gate_signs = jnp.where(jnp.arange(GATES, dtype=jnp.int32) % 2 == 0, 1.0, -1.0).astype(jnp.float32)

    def one_gate(totals, inputs):
        gate_now, mid_point, speed, conductance, reversal, direction = inputs
        shifted = voltage - mid_point
        steady = jax.nn.sigmoid(direction * gate_slope * shifted)
        decay_factor = jnp.exp(-time_step * speed * (1.0 + jax.nn.sigmoid(shifted)))
        renewed = steady + (gate_now - steady) * decay_factor
        return (totals[0] + conductance * renewed, totals[1] + (conductance * reversal) * renewed), renewed

    zero_field = jnp.zeros_like(voltage)
    sums, renewed_all = lax.scan(one_gate, (zero_field, zero_field), (gates, gate_half, gate_rate, gate_cond, gate_rev, gate_signs))
    ionic = voltage * sums[0] - sums[1]
    return renewed_all, ionic


def line_count(length):
    places = jnp.arange(length, dtype=jnp.int32)
    return (places > 0).astype(jnp.float32) + (places < length - 1).astype(jnp.float32)


def reference(tissue_v, tissue_gates, tissue_diff, fibre_v, fibre_gates, fibre_diff, gate_half, gate_rate, gate_cond, gate_rev, junc_cond, junc_fibre, junc_fcell, junc_owner, junc_tcell, junc_class):
    depth_all, height_all, width_all = tissue_v.shape
    fibre_total, fibre_len = fibre_v.shape
    share = fibre_len // N_PLANE
    total_junctions = junc_fibre.shape[0]
    holder = jnp.arange(total_junctions, dtype=jnp.int32) // JUNC_DEV
    fibre_row = (holder // N_PLANE) * FIB_DEV + junc_fibre
    fibre_col = (holder % N_PLANE) * share + junc_fcell
    fibre_flat = (fibre_row * fibre_len + fibre_col).astype(jnp.int32)
    owners = junc_owner[:, 0]
    layer_z = (owners // N_PLANE) * CZ + junc_tcell // (CY * NX)
    row_y = (owners % N_PLANE) * CY + (junc_tcell // NX) % CY
    tissue_flat = ((layer_z * height_all + row_y) * width_all + junc_tcell % NX).astype(jnp.int32)
    coupling = jnp.sum(jnp.where(junc_class[:, None] == jnp.arange(CLASSES, dtype=jnp.int32)[None, :], junc_cond[None, :], jnp.zeros((), jnp.float32)), axis=1)
    tissue_count = line_count(depth_all)[:, None, None] + line_count(height_all)[None, :, None] + line_count(width_all)[None, None, :]
    fibre_count = line_count(fibre_len)[None, :]

    def advance(carry, unused):
        tissue_now, tissue_state, fibre_now, fibre_state = carry
        tissue_line = tissue_now.reshape(-1)
        fibre_line = fibre_now.reshape(-1)
        current = coupling * (fibre_line[fibre_flat] - tissue_line[tissue_flat])
        tissue_source = jnp.zeros_like(tissue_line).at[tissue_flat].add(current).reshape(tissue_now.shape)
        fibre_source = jnp.zeros_like(fibre_line).at[fibre_flat].add(-current).reshape(fibre_now.shape)
        padded = jnp.pad(tissue_now, 1)
        neighbours = padded[2:, 1:-1, 1:-1] + padded[:-2, 1:-1, 1:-1] + padded[1:-1, 2:, 1:-1] + padded[1:-1, :-2, 1:-1] + padded[1:-1, 1:-1, 2:] + padded[1:-1, 1:-1, :-2]
        tissue_lap = neighbours - tissue_count * tissue_now
        fibre_padded = jnp.pad(fibre_now, ((0, 0), (1, 1)))
        fibre_lap = fibre_padded[:, 2:] + fibre_padded[:, :-2] - fibre_count * fibre_now
        tissue_state, tissue_ionic = membrane(tissue_now, tissue_state, gate_half, gate_rate, gate_cond, gate_rev)
        fibre_state, fibre_ionic = membrane(fibre_now, fibre_state, gate_half, gate_rate, gate_cond, gate_rev)
        tissue_next = tissue_now + time_step * (tissue_diff * tissue_lap - tissue_ionic + tissue_source)
        fibre_next = fibre_now + time_step * (fibre_diff * fibre_lap - fibre_ionic + fibre_source)
        return (tissue_next, tissue_state, fibre_next, fibre_state), None

    final, unused_out = lax.scan(advance, (tissue_v, tissue_gates, fibre_v, fibre_gates), None, length=STEPS)
    return final[0], final[2]
```

```python
import jax
import jax.numpy as jnp
from jax import lax
from jax.experimental import pallas as pl
from jax.experimental.pallas import tpu as pltpu
from jax.sharding import PartitionSpec as P

STEPS = 14
DT = 0.1
LN = 128
NV = 8
ROWS = 64
BLOCK = 2
VLIMIT = 8 * 1024 * 1024


def lane_iota():
    return lax.broadcasted_iota(jnp.int32, (8, LN), 1)


def sub_iota():
    return lax.broadcasted_iota(jnp.int32, (8, LN), 0)


def take(source, lanes):
    return jnp.take_along_axis(source, lanes, axis=1, mode="promise_in_bounds")


def gather_pair(tables, rows_refs, lane_refs, emit):
    def block(i, carry):
        for u in range(BLOCK):
            v = i * BLOCK + u
            at = pl.ds(pl.multiple_of(v * 8, 8), 8)
            for k, load in enumerate(tables):
                rows = rows_refs[k][at, :]
                lanes = lane_refs[k][at, :]
                total = jnp.zeros((8, LN), jnp.float32)
                for r in range(ROWS):
                    got = take(jnp.broadcast_to(load(r), (8, LN)), lanes)
                    total = jnp.where(rows == r, got, total)
                emit(k, v, at, total)
        return carry

    lax.fori_loop(0, NV // BLOCK, block, 0)


def plain_row(ref):
    return lambda r: ref[r : r + 1, :]


def fibre_row(ref):
    def load(r):
        f = (r // 32) * 8 + r % 8
        q = (r // 8) % 4
        return ref[f : f + 1, q * LN : (q + 1) * LN]

    return load


def step_eight(x, sub):
    turned = pltpu.roll(x, 1, axis=0)
    return jnp.where(sub == 0, pltpu.roll(turned, 1, axis=1), turned)


def earlier(values, k, sub):
    if k < 3:
        q = 1 << k
        return [values[v - q] if v >= q else step_eight(values[v - q + 8], sub) for v in range(NV)]
    if k < 6:
        q = 1 << (k - 3)
        out = []
        for x in values:
            turned = pltpu.roll(x, q, axis=0)
            out.append(jnp.where(sub < q, pltpu.roll(turned, 1, axis=1), turned))
        return out
    return [pltpu.roll(x, 1 << (k - 6), axis=1) for x in values]


def scan_steps(values, offs, ks, sub):
    for k in ks:
        before = earlier(values, k, sub)
        values = [x + jnp.where(o >= (1 << k), b, 0.0) for x, o, b in zip(values, offs, before)]
    return values


def load_list(ref):
    return [ref[8 * v : 8 * v + 8, :] for v in range(NV)]


def store_list(ref, values):
    for v, x in enumerate(values):
        ref[8 * v : 8 * v + 8, :] = x


def segment_sums(slot_refs, srow, slane, off, erow, elane, work, emit):
    tables = [plain_row(ref) for ref in slot_refs]

    def keep(k, v, at, total):
        work[k][at, :] = total

    gather_pair(tables, srow, slane, keep)
    sub = sub_iota()
    for k, ref in enumerate(work):
        offs = load_list(off[k])
        store_list(ref, scan_steps(load_list(ref), offs, range(3), sub))
        longest = offs[0]
        for o in offs[1:]:
            longest = jnp.maximum(longest, o)

        @pl.when(jnp.max(longest) >= 8)
        def _(ref=ref, offs=offs):
            store_list(ref, scan_steps(load_list(ref), offs, range(3, 13), sub))

    gather_pair([plain_row(ref) for ref in work], erow, elane, emit)


def sort_positions(values, lane, sub):
    def bit_mask(m):
        if m < 3:
            return None
        return ((sub >> (m - 3)) & 1) == 1 if m < 6 else ((lane >> (m - 6)) & 1) == 1

    for m in range(1, 14):
        for b in range(m - 1, -1, -1):
            down = bit_mask(m) if 3 <= m < 13 else None
            if b < 3:
                out = list(values)
                for v in range(NV):
                    w = v | (1 << b)
                    if v == w:
                        continue
                    lo = jnp.minimum(values[v], values[w])
                    hi = jnp.maximum(values[v], values[w])
                    if down is not None:
                        out[v] = jnp.where(down, hi, lo)
                        out[w] = jnp.where(down, lo, hi)
                    elif m < 3 and (v >> m) & 1:
                        out[v], out[w] = hi, lo
                    else:
                        out[v], out[w] = lo, hi
                values = out
            else:
                axis = 0 if b < 6 else 1
                d = 1 << (b - 3) if b < 6 else 1 << (b - 6)
                size = 8 if b < 6 else LN
                upper = bit_mask(b)
                keep_high = upper if down is None else jnp.logical_xor(upper, down)
                out = []
                for x in values:
                    partner = jnp.where(upper, pltpu.roll(x, d, axis=axis), pltpu.roll(x, size - d, axis=axis))
                    out.append(jnp.where(keep_high, jnp.maximum(x, partner), jnp.minimum(x, partner)))
                values = out
    return values


def prep_kernel(cell, gain, count, srow, slane, off, erow, elane, total, work):
    lane, sub = lane_iota(), sub_iota()
    cells = load_list(cell)
    keys = []
    for v in range(NV):
        slot = (v * 8 + sub) * LN + lane
        keys.append(jnp.where(cells[v] < 0, ROWS * LN, cells[v]) * (ROWS * LN) + slot)
    keys = sort_positions(keys, lane, sub)
    slots = [x & (ROWS * LN - 1) for x in keys]
    store_list(srow, [x >> 7 for x in slots])
    store_list(slane, [x & (LN - 1) for x in slots])
    owner = [x >> 13 for x in keys]
    place = [v + 8 * sub + 64 * lane for v in range(NV)]
    before = earlier(owner, 0, sub)
    first = [jnp.where((o != b) | (p == 0), p, 0) for o, b, p in zip(owner, before, place)]
    for k in range(13):
        prior = earlier(first, k, sub)
        first = [jnp.maximum(x, jnp.where(p >= (1 << k), y, 0)) for x, y, p in zip(first, prior, place)]
    filled = [o < ROWS * LN for o in owner]
    store_list(off, [jnp.where(ok, p - f, 0) for ok, p, f in zip(filled, place, first)])

    counts = load_list(count)
    run = []
    for x in counts:
        for k in range(7):
            x = x + jnp.where(lane >= (1 << k), pltpu.roll(x, 1 << k, axis=1), 0)
        run.append(x)
    base = jnp.zeros((8, LN), jnp.int32)
    ends_row, ends_lane = [], []
    for v in range(NV):
        rowsum = jnp.broadcast_to(run[v][:, LN - 1 :], (8, LN))
        upto = rowsum
        for k in range(3):
            upto = upto + jnp.where(sub >= (1 << k), pltpu.roll(upto, 1 << k, axis=0), 0)
        last = run[v] + upto - rowsum + base - 1
        ends_row.append(jnp.where(counts[v] > 0, 8 * (last & 7) + ((last >> 3) & 7), -1))
        ends_lane.append(jnp.where(counts[v] > 0, last >> 6, 0))
        base = base + jnp.broadcast_to(upto[7:8, :], (8, LN))
    store_list(erow, ends_row)
    store_list(elane, ends_lane)

    def emit(k, v, at, value):
        total[at, :] = value

    segment_sums([gain], [srow], [slane], [off], [erow], [elane], [work], emit)


def vspec():
    return pl.BlockSpec(memory_space=pltpu.VMEM)


def sspec():
    return pl.BlockSpec(memory_space=pltpu.SMEM)


def f32(*shape):
    return jax.ShapeDtypeStruct(shape, jnp.float32)


def i32(*shape):
    return jax.ShapeDtypeStruct(shape, jnp.int32)


def call(kernel, name, outs, specs, scratch=(), aliases=None):
    return pl.pallas_call(
        kernel,
        name=name,
        out_shape=outs,
        in_specs=specs,
        out_specs=tuple(vspec() for _ in outs),
        scratch_shapes=list(scratch),
        input_output_aliases=aliases or {},
        compiler_params=pltpu.CompilerParams(vmem_limit_bytes=VLIMIT),
    )


def prepare(cell, gain, count):
    table = i32(ROWS, LN)
    return call(
        prep_kernel,
        "prep",
        (table, table, table, table, table, f32(ROWS, LN)),
        [vspec()] * 3,
        [pltpu.VMEM((ROWS, LN), jnp.float32)],
    )(cell, gain, count)


def emit_messages(vt, vf, frow, flane, crow, clane, gslot, send, zup, zdn, yup, ydn):
    lane = lane_iota()
    parts = {}

    def emit(k, v, at, value):
        high = pl.ds(pl.multiple_of(v * 8 + ROWS, 8), 8)
        if k == 0:
            parts["fibre"] = value * gslot[at, :]
            return
        fib = parts["fibre"]
        send[at, :] = jnp.where(lane < 64, fib, pltpu.roll(value, 64, axis=1))
        send[high, :] = jnp.where(lane < 64, pltpu.roll(fib, 64, axis=1), value)

    gather_pair([fibre_row(vf), plain_row(vt)], [frow, crow], [flane, clane], emit)
    zup[...] = vt[48:64, :]
    zdn[...] = vt[0:16, :]
    yup[0:16, :] = vf[:, 384:512]
    ydn[0:16, :] = vf[:, 0:128]
    for z in range(4):
        yup[16 + z : 17 + z, :] = vt[16 * z + 15 : 16 * z + 16, :]
        ydn[16 + z : 17 + z, :] = vt[16 * z : 16 * z + 1, :]
    yup[20:24, :] = jnp.zeros((4, LN), jnp.float32)
    ydn[20:24, :] = jnp.zeros((4, LN), jnp.float32)


def first_kernel(vt, vf, frow, flane, crow, clane, gslot, send, zup, zdn, yup, ydn):
    emit_messages(vt, vf, frow, flane, crow, clane, gslot, send, zup, zdn, yup, ydn)


def exchange_kernel(
    recv, pt, pf, gslot,
    t_srow, t_slane, t_off, t_erow, t_elane,
    f_srow, f_slane, f_off, f_erow, f_elane,
    frow, flane, crow, clane,
    vt, vf, send, zup, zdn, yup, ydn,
    slot_t, slot_f, work_t, work_f,
):
    lane = lane_iota()
    for v in range(NV):
        low = recv[8 * v : 8 * v + 8, :]
        high = recv[ROWS + 8 * v : ROWS + 8 * v + 8, :]
        slot_t[8 * v : 8 * v + 8, :] = jnp.where(lane < 64, low, pltpu.roll(high, 64, axis=1))
        slot_f[8 * v : 8 * v + 8, :] = jnp.where(lane < 64, pltpu.roll(low, 64, axis=1), high) * gslot[8 * v : 8 * v + 8, :]

    def emit(k, v, at, value):
        if k == 0:
            vt[at, :] = pt[at, :] + DT * value
        else:
            fib = pl.ds(pl.multiple_of((v // 4) * 8, 8), 8)
            col = pl.ds(pl.multiple_of((v % 4) * LN, LN), LN)
            vf[fib, col] = pf[fib, col] + DT * value

    segment_sums(
        [slot_t, slot_f], [t_srow, f_srow], [t_slane, f_slane], [t_off, f_off],
        [t_erow, f_erow], [t_elane, f_elane], [work_t, work_f], emit,
    )
    emit_messages(vt, vf, frow, flane, crow, clane, gslot, send, zup, zdn, yup, ydn)


MESSAGES = (f32(128, LN), f32(16, LN), f32(16, LN), f32(24, LN), f32(24, LN))


def membrane_kernel(par, vt, vf, gt_in, gf_in, gt, gf, ion_t, ion_f):
    def one(v, old, k):
        gate = old
        t1 = jnp.tanh(0.5 * v - par[0, k])
        th = jnp.tanh(v - par[1, k])
        steady = 0.5 + (0.5 if k % 2 == 0 else -0.5) * th
        factor = jnp.exp2(par[2, k] + par[3, k] * t1)
        return steady + (gate - steady) * factor

    def block(b, carry):
        at = pl.ds(pl.multiple_of(b * 8, 8), 8)
        fib = pl.ds(pl.multiple_of((b // 4) * 8, 8), 8)
        col = pl.ds(pl.multiple_of((b % 4) * LN, LN), LN)
        v = vt[at, :]
        w = vf[fib, col]
        st = jnp.zeros((8, LN), jnp.float32)
        dt_ = st
        sf = st
        df = st
        for k in range(gt.shape[0]):
            a = one(v, gt_in[k, at, :], k)
            gt[k, at, :] = a
            st = st + par[4, k] * a
            dt_ = dt_ + par[5, k] * a
            c = one(w, gf_in[k, fib, col], k)
            gf[k, fib, col] = c
            sf = sf + par[4, k] * c
            df = df + par[5, k] * c
        ion_t[at, :] = v * st - dt_
        ion_f[fib, col] = w * sf - df
        return carry

    lax.fori_loop(0, NV, block, 0)


def combine_kernel(edge, vt, vf, ion_t, ion_f, diff_t, diff_f, sum_t, sum_f, zlo, zhi, ylo, yhi, pt, pf):
    lane = lax.broadcasted_iota(jnp.int32, (16, LN), 1)
    row = lax.broadcasted_iota(jnp.int32, (16, LN), 0)
    not_first = jnp.where(lane > 0, 1.0, 0.0)
    not_last = jnp.where(lane < LN - 1, 1.0, 0.0)
    for z in range(4):
        here = vt[16 * z : 16 * z + 16, :]
        below = vt[16 * z - 16 : 16 * z, :] if z > 0 else zlo[...] * edge[0]
        above = vt[16 * z + 16 : 16 * z + 32, :] if z < 3 else zhi[...] * edge[1]
        front = jnp.broadcast_to(ylo[16 + z : 17 + z, :] * edge[2], (16, LN))
        back = jnp.broadcast_to(yhi[16 + z : 17 + z, :] * edge[3], (16, LN))
        left_y = jnp.where(row == 0, front, pltpu.roll(here, 1, axis=0))
        right_y = jnp.where(row == 15, back, pltpu.roll(here, 15, axis=0))
        left_x = pltpu.roll(here, 1, axis=1) * not_first
        right_x = pltpu.roll(here, LN - 1, axis=1) * not_last
        count = not_first + not_last + jnp.where(row == 0, edge[2], 1.0) + jnp.where(row == 15, edge[3], 1.0)
        count = count + (edge[0] if z == 0 else 1.0) + (edge[1] if z == 3 else 1.0)
        lap = below + above + left_y + right_y + left_x + right_x - count * here
        at = slice(16 * z, 16 * z + 16)
        pt[at, :] = here + DT * (diff_t[at, :] * lap - ion_t[at, :] - sum_t[at, :] * here)
    for q in range(4):
        at = slice(q * LN, (q + 1) * LN)
        here = vf[:, at]
        prior = vf[:, (q - 1) * LN : q * LN] if q > 0 else ylo[0:16, :] * edge[2]
        after = vf[:, (q + 1) * LN : (q + 2) * LN] if q < 3 else yhi[0:16, :] * edge[3]
        left = jnp.where(lane == 0, pltpu.roll(prior, 1, axis=1), pltpu.roll(here, 1, axis=1))
        right = jnp.where(lane == LN - 1, pltpu.roll(after, LN - 1, axis=1), pltpu.roll(here, LN - 1, axis=1))
        count = jnp.full((16, LN), 2.0, jnp.float32)
        if q == 0:
            count = count - jnp.where(lane == 0, 1.0 - edge[2], 0.0)
        if q == 3:
            count = count - jnp.where(lane == LN - 1, 1.0 - edge[3], 0.0)
        lap = left + right - count * here
        fsum = jnp.concatenate([sum_f[8 * q : 8 * q + 8, :], sum_f[32 + 8 * q : 40 + 8 * q, :]], axis=0)
        pf[:, at] = here + DT * (diff_f[:, at] * lap - ion_f[:, at] - fsum * here)


def make_onehot(indices, count):
    return (indices[:, None] == jnp.arange(count, dtype=jnp.int32)[None, :]).astype(jnp.float32)


def place_values(row_onehot, col_onehot, values):
    return lax.dot_general(
        row_onehot, col_onehot * values[:, None], (((0,), (0,)), ((), ())),
        precision=lax.Precision.HIGHEST, preferred_element_type=jnp.float32,
    )


def cell_counts(cells):
    rows = jnp.where(cells < 0, -1, cells // LN).reshape(-1)
    cols = jnp.where(cells < 0, -1, cells % LN).reshape(-1)
    counts = lax.dot_general(
        make_onehot(rows, ROWS), make_onehot(cols, LN), (((0,), (0,)), ((), ())),
        preferred_element_type=jnp.float32,
    )
    return counts.astype(jnp.int32)


def fold(pairs):
    return jnp.concatenate([pairs[:64], pairs[64:]], axis=1)


def split_cells(cells):
    return jnp.where(cells < 0, -1, cells >> 7), jnp.where(cells < 0, 0, cells & (LN - 1))


def body(
    tissue_v, tissue_gates, tissue_diff, fibre_v, fibre_gates, fibre_diff,
    gate_half, gate_rate, gate_cond, gate_rev, junc_cond,
    junc_fibre, junc_fcell, junc_owner, junc_tcell, junc_class,
):
    slabs = lax.axis_size("slab")
    planes = lax.axis_size("plane")
    devices = slabs * planes
    gates = tissue_gates.shape[0]
    capacity = 64
    vt = tissue_v.reshape(ROWS, LN)
    diff_t = tissue_diff.reshape(ROWS, LN)
    gt = tissue_gates.reshape(gates, ROWS, LN)

    owners = junc_owner[:, 0]
    owner_onehot = make_onehot(owners, devices)
    owner_table = owner_onehot.astype(jnp.int32)
    rank = jnp.sum(jnp.cumsum(owner_table, axis=0) * owner_table, axis=1) - 1
    rank_onehot = make_onehot(rank, capacity)
    gain = jnp.sum(
        jnp.where(
            junc_class[:, None] == jnp.arange(junc_cond.shape[0], dtype=jnp.int32)[None, :],
            junc_cond[None, :], jnp.zeros((), jnp.float32),
        ),
        axis=1,
    )
    fibre_id = ((junc_fibre // 8) * 32 + (junc_fcell // LN) * 8 + junc_fibre % 8) * LN + junc_fcell % LN
    slot_fibre = place_values(owner_onehot, rank_onehot, (fibre_id + 1).astype(jnp.float32))
    slot_cell = place_values(owner_onehot, rank_onehot, (junc_tcell + 1).astype(jnp.float32))
    slot_gain = place_values(owner_onehot, rank_onehot, gain)
    sent = jnp.concatenate([slot_cell, slot_gain], axis=1)
    got = lax.all_to_all(sent, ("slab", "plane"), split_axis=0, concat_axis=0, tiled=True)

    fcells = fold(slot_fibre).astype(jnp.int32) - 1
    gslot = fold(slot_gain)
    frow, flane = split_cells(fcells)
    f_srow, f_slane, f_off, f_erow, f_elane, sum_f = prepare(fcells, gslot, cell_counts(fcells))
    tcells = fold(got[:, :64]).astype(jnp.int32) - 1
    tgain = fold(got[:, 64:])
    crow, clane = split_cells(tcells)
    t_srow, t_slane, t_off, t_erow, t_elane, sum_t = prepare(tcells, tgain, cell_counts(tcells))

    log2e = 1.4426950408889634
    par = jnp.stack(
        [
            0.5 * gate_half, gate_half,
            (-1.5 * DT * log2e) * gate_rate, (-0.5 * DT * log2e) * gate_rate,
            gate_cond, gate_cond * gate_rev,
        ]
    )
    s, p = lax.axis_index("slab"), lax.axis_index("plane")
    edge = jnp.stack([s > 0, s < slabs - 1, p > 0, p < planes - 1]).astype(jnp.float32)

    def ring(axis, shift):
        n = lax.axis_size(axis)
        return [(i, (i + shift) % n) for i in range(n)]

    messages = call(first_kernel, "first", MESSAGES, [vspec()] * 7)(vt, fibre_v, frow, flane, crow, clane, gslot)

    def advance(i, carry):
        vt, vf, gt, gf, send, zup, zdn, yup, ydn = carry
        recv = lax.all_to_all(send, ("slab", "plane"), split_axis=0, concat_axis=0, tiled=True)
        zlo = lax.ppermute(zup, "slab", ring("slab", 1))
        zhi = lax.ppermute(zdn, "slab", ring("slab", -1))
        ylo = lax.ppermute(yup, "plane", ring("plane", 1))
        yhi = lax.ppermute(ydn, "plane", ring("plane", -1))
        gt, gf, ion_t, ion_f = call(
            membrane_kernel, "membrane",
            (f32(gates, ROWS, LN), f32(gates, 16, 512), f32(ROWS, LN), f32(16, 512)),
            [sspec()] + [vspec()] * 4, aliases={3: 0, 4: 1},
        )(par, vt, vf, gt, gf)
        pt, pf = call(
            combine_kernel, "combine", (f32(ROWS, LN), f32(16, 512)), [sspec()] + [vspec()] * 12
        )(edge, vt, vf, ion_t, ion_f, diff_t, fibre_diff, sum_t, sum_f, zlo, zhi, ylo, yhi)
        out = call(
            exchange_kernel, "exchange", (f32(ROWS, LN), f32(16, 512)) + MESSAGES, [vspec()] * 18,
            [pltpu.VMEM((ROWS, LN), jnp.float32)] * 4,
        )(
            recv, pt, pf, gslot,
            t_srow, t_slane, t_off, t_erow, t_elane,
            f_srow, f_slane, f_off, f_erow, f_elane,
            frow, flane, crow, clane,
        )
        return (out[0], out[1], gt, gf) + tuple(out[2:])

    final = lax.fori_loop(0, STEPS, advance, (vt, fibre_v, gt, fibre_gates) + tuple(messages))
    return final[0].reshape(tissue_v.shape), final[1]


def solution(mesh):
    in_specs = (
        P("slab", "plane", None),
        P(None, "slab", "plane", None),
        P("slab", "plane", None),
        P("slab", "plane"),
        P(None, "slab", "plane"),
        P("slab", "plane"),
        P(),
        P(),
        P(),
        P(),
        P(),
        P(("slab", "plane")),
        P(("slab", "plane")),
        P(("slab", "plane"), None),
        P(("slab", "plane")),
        P(("slab", "plane")),
    )
    out_specs = (P("slab", "plane", None), P("slab", "plane"))
    return jax.shard_map(body, mesh=mesh, in_specs=in_specs, out_specs=out_specs, check_vma=False)
```
